32 devices in a mesh: groups: 2 (over y), ep: 4 (over z), dp: 4 (over x, core), tp: 1.
Axes of the slice: x: 2, y: 2, z: 4, core: 2. Of those that a mesh axis runs over, the one named last changes fastest.
Arguments:
- tokens: bfloat16 [2048, 2048], P(('groups', 'ep', 'dp', 'tp')), parts along dimension 0, may hold values from -6 to 6
- experts_one: int32 [2048, 8], P(('groups', 'ep', 'dp', 'tp')), parts along dimension 0, may hold values from 0 to 15, all different within a row; in each aligned block of 64 rows (0 to 63, 64 to 127, ...) at most 40 rows name the same one
- gates_one: float32 [2048, 8], P(('groups', 'ep', 'dp', 'tp')), parts along dimension 0, may hold values from 0.05 to 0.5
- w_in_one: bfloat16 [16, 2048, 2, 768], P(('ep', 'dp'), None, None, 'tp'), may hold values from -0.125 to 0.125
- w_down_one: bfloat16 [16, 768, 2048], P(('ep', 'dp'), 'tp'), may hold values from -0.21875 to 0.21875
- norm_gain: float32 [2048], replicated, may hold values from 0.5 to 1.5
- experts_two: int32 [2048, 8], P(('groups', 'ep', 'dp', 'tp')), parts along dimension 0, may hold values from 0 to 15, all different within a row; in each aligned block of 64 rows (0 to 63, 64 to 127, ...) at most 40 rows name the same one
- gates_two: float32 [2048, 8], P(('groups', 'ep', 'dp', 'tp')), parts along dimension 0, may hold values from 0.05 to 0.5
- placement_two: int32 [16], replicated, may hold values from 0 to 15, each once
- w_in_two: bfloat16 [16, 2048, 2, 768], P(('ep', 'dp'), None, None, 'tp'), may hold values from -0.125 to 0.125
- w_down_two: bfloat16 [16, 768, 2048], P(('ep', 'dp'), 'tp'), may hold values from -0.21875 to 0.21875
Outputs:
- layer_out: bfloat16 [2048, 2048], P(('groups', 'ep', 'dp', 'tp')), parts along dimension 0
The draws below stay inside these ranges and needn't reach their ends.
There are 2 independent parts, one for each index of `groups`. The reference program is written for one: setup_inputs(seed, part) draws one part's arguments, and reference() takes and returns one part's arrays. A program takes and returns all parts, laid end to end along the dimension named above; an argument that names none is the same for every part. Nothing has to cross between parts.
Inputs may be any that keep to these rules, and one draw needn't show every extreme that they name: `experts_one`: each token names 8 different experts; among the 64 tokens of one device no expert is named more than 40 times, and on some device some expert is named exactly 40 times. `experts_two`: each token names 8 different experts; among the 64 tokens of one device no expert is named more than 40 times, and on some device some expert is named exactly 40 times. `placement_two`: each slot is named by exactly one expert.
All inputs are finite; a program needn't handle non-finite values.
Results may differ from the reference program's by a relative error of at most 0.011.
Values may be sent and summed in bfloat16 or wider, within the bound.
A program may use at most 128 MiB of HBM per device.

```python
import math
import jax
import jax.numpy as jnp
import numpy as np
from jax import lax

D = 2048
FF = 768
TOPK = 8
TOK_DEV = 64
EXPERTS = 16
MOST = 40
TOKENS = 1024
N_EP = 4
N_DP = 4
N_TP = 1


def shard_levels(key, dims, cuts, smallest, top_value):
    loudness, own = 1.0, jax.random.fold_in(key, 6)
    for position, parts in cuts:
        heights = jnp.exp(jax.random.uniform(jax.random.fold_in(own, position), (parts,), jnp.float32, smallest / len(cuts), top_value / len(cuts)))
        loudness = loudness * jnp.repeat(heights, dims[position] // parts).reshape([-1 if axis == position else 1 for axis in range(len(dims))])
    return loudness


def assign_block(stream_key, own, number, rows, count, top, limit, lean):
    sequence = jax.random.permutation(stream_key, count)
    crowded, common = shares(count, rows * top, limit, lean, True), shares(count, rows * top, limit, lean, False)
    places = jnp.arange(count)

    def named(sizes, rotation):
        used = int((sizes > 0).sum())
        fixed = max(1, used // 4)
        passed = fixed + (places - fixed + rotation * (used - fixed)) % max(1, count - fixed)
        return jnp.zeros((count,), jnp.int32).at[sequence[jnp.where(places < fixed, places, passed)]].set(jnp.asarray(sizes, jnp.int32))

    sizes = jnp.where(number % 4 == 0, named(crowded, number // 4), named(common, number - number // 4 - 1))
    mixed = jax.random.permutation(jax.random.fold_in(own, 3), count)
    giver, receiver = mixed[0:count // 2 * 2:2], mixed[1:count // 2 * 2:2]
    margin = jnp.minimum(sizes[giver] - 1, limit - sizes[receiver]) // 2
    margin = jnp.where((giver == sequence[0]) | (receiver == sequence[0]) | (sizes[receiver] == 0), 0, jnp.maximum(margin, 0))
    passed = jax.random.randint(jax.random.fold_in(own, 4), (count // 2,), 0, 1 << 20) % (margin + 1)
    sizes = sizes.at[giver].add(-passed).at[receiver].add(passed)
    labels = jnp.searchsorted(jnp.cumsum(sizes), jnp.arange(rows * top), side="right").astype(jnp.int32)
    listing = labels.reshape(top, rows).T
    listing = listing[jax.random.permutation(jax.random.fold_in(own, 1), rows)]
    rotation = jax.random.randint(jax.random.fold_in(own, 2), (rows, 1), 0, top)
    return jnp.take_along_axis(listing, (jnp.arange(top)[None, :] + rotation) % top, axis=1)


def shares(count, total, bound, lean, full):
    weights = [(1 << 20) // math.isqrt(rank ** lean) + 1 for rank in range(1, count + 1)]
    largest = bound if full else min(bound, max(-(-total // count), total * weights[0] // sum(weights)))
    least = 1 if total - largest >= count - 1 else 0
    holding, spare = [largest] + [least] * (count - 1), total - largest - least * (count - 1)
    while spare > 0:
        candidates = [i for i in range(1, count) if holding[i] < largest] or [i for i in range(1, count) if holding[i] < bound]
        whole, remaining = sum([weights[i] for i in candidates]), spare
        for i in candidates:
            more = min(bound - holding[i], max(1, remaining * weights[i] // whole), spare)
            holding[i] = holding[i] + more
            spare = spare - more
    return np.array(holding)


def gaussian(own_key, extent, scale, reach, cuts=(), kind=jnp.bfloat16):
    entries = jax.random.normal(own_key, extent, jnp.float32) * scale
    if len(cuts) > 0:
        entries = shard_levels(own_key, extent, cuts, -0.22, 0.18) * entries
    return jnp.clip(entries, min=-reach, max=reach).astype(kind)


def setup_inputs(seed: int = 0, part: int = 0) -> dict:
    key_of = jax.random.split(jax.random.key(seed), 12)
    part_splits = jax.random.split(jax.random.fold_in(key_of[11], part), 12)
    tokens = gaussian(part_splits[0], (TOKENS, D), 1.0, 6.0, ((0, 16),))
    experts_one_keys = jax.random.split(jax.random.fold_in(part_splits[1], 1), TOKENS // TOK_DEV)
    experts_one_turns = jax.random.permutation(jax.random.fold_in(part_splits[1], 3), TOKENS // TOK_DEV)
    experts_one = jax.vmap(lambda own, number: assign_block(jax.random.fold_in(part_splits[1], 2), own, number, TOK_DEV, EXPERTS, TOPK, MOST, 2))(experts_one_keys, experts_one_turns).reshape((TOKENS, TOPK))
    gates_one = jnp.clip(jnp.exp(math.log(0.5) - 2.3025851 * jax.random.uniform(part_splits[2], (TOKENS, TOPK), jnp.float32) ** shard_levels(part_splits[2], (TOKENS, TOPK), ((0, 16),), -0.2, 0.2)), 0.05, 0.5)
    w_in_one = gaussian(key_of[3], (EXPERTS, D, 2, FF), D ** -0.5, 0.125, ((0, 16),))
    w_down_one = gaussian(key_of[4], (EXPERTS, FF, D), FF ** -0.5, 0.21875, ((0, 16),))
    norm_gain = jnp.clip(1.0 + 0.1 * jax.random.normal(key_of[5], (D,), jnp.float32), 0.5, 1.5)
    experts_two_keys = jax.random.split(jax.random.fold_in(part_splits[6], 1), TOKENS // TOK_DEV)
    experts_two_turns = jax.random.permutation(jax.random.fold_in(part_splits[6], 3), TOKENS // TOK_DEV)
    experts_two = jax.vmap(lambda own, number: assign_block(jax.random.fold_in(part_splits[6], 2), own, number, TOK_DEV, EXPERTS, TOPK, MOST, 2))(experts_two_keys, experts_two_turns).reshape((TOKENS, TOPK))
    gates_two = jnp.clip(jnp.exp(math.log(0.5) - 2.3025851 * jax.random.uniform(part_splits[7], (TOKENS, TOPK), jnp.float32) ** shard_levels(part_splits[7], (TOKENS, TOPK), ((0, 16),), -0.2, 0.2)), 0.05, 0.5)
    placement_two = jax.random.permutation(key_of[8], EXPERTS).astype(jnp.int32)
    w_in_two = gaussian(key_of[9], (EXPERTS, D, 2, FF), D ** -0.5, 0.125, ((0, 16),))
    w_down_two = gaussian(key_of[10], (EXPERTS, FF, D), FF ** -0.5, 0.21875, ((0, 16),))
    return dict(tokens=tokens, experts_one=experts_one, gates_one=gates_one, w_in_one=w_in_one, w_down_one=w_down_one, norm_gain=norm_gain, experts_two=experts_two, gates_two=gates_two, placement_two=placement_two, w_in_two=w_in_two, w_down_two=w_down_two)


def expert_layer(rows_in, layer_slots, gate_values, w_in, w_down):
    token_count, top_count = layer_slots.shape
    expert_total, row_width, pair_n, hidden_n = w_in.shape
    slot_cap = MOST * N_EP * N_DP * N_TP
    block_width = hidden_n // N_TP
    flat_ids = layer_slots.reshape(-1)
    owner_row = jnp.arange(token_count * top_count, dtype=jnp.int32) // top_count
    flat_gates = gate_values.reshape(-1)

    def accumulate(summed, expert_id):
        hit_mask = flat_ids == expert_id
        slot_rank = jnp.cumsum(hit_mask.astype(jnp.int32)) - 1
        slot_pos = jnp.where(hit_mask, slot_rank, slot_cap).astype(jnp.int32)
        picked = jnp.zeros((slot_cap,), jnp.int32).at[slot_pos].set(owner_row, mode='drop')
        weight = jnp.zeros((slot_cap,), jnp.float32).at[slot_pos].set(flat_gates, mode='drop')
        chosen = rows_in[picked]
        gate_up = jnp.dot(chosen, w_in[expert_id].reshape(row_width, pair_n * hidden_n), preferred_element_type=jnp.float32)
        activated = (jax.nn.silu(gate_up[:, :hidden_n]) * gate_up[:, hidden_n:]).astype(jnp.bfloat16)
        down_now = w_down[expert_id]
        total = jnp.zeros((slot_cap, row_width), jnp.float32)
        for block in range(N_TP):
            lo_unit = block * block_width
            partial_out = jnp.dot(activated[:, lo_unit:lo_unit + block_width], down_now[lo_unit:lo_unit + block_width], preferred_element_type=jnp.float32)
            total = total + partial_out.astype(jnp.bfloat16).astype(jnp.float32)
        expert_out = total.astype(jnp.bfloat16)
        summed = summed.at[picked].add(weight[:, None] * expert_out.astype(jnp.float32))
        return (summed, None)
    start_sum = jnp.zeros((token_count, row_width), jnp.float32)
    summed, _ = lax.scan(accumulate, start_sum, jnp.arange(expert_total, dtype=jnp.int32))
    return summed

def reference(tokens, experts_one, gates_one, w_in_one, w_down_one, norm_gain, experts_two, gates_two, placement_two, w_in_two, w_down_two):
    moe_one = expert_layer(tokens, experts_one, gates_one, w_in_one, w_down_one)
    mixed = (tokens.astype(jnp.float32) + moe_one).astype(jnp.bfloat16)
    mixed = lax.optimization_barrier(mixed)
    mixed_wide = mixed.astype(jnp.float32)
    inv_rms = lax.rsqrt(lax.optimization_barrier(jnp.mean(mixed_wide * mixed_wide, axis=1, keepdims=True)) + 1e-06)
    normed = (mixed_wide * inv_rms * norm_gain[None, :]).astype(jnp.bfloat16)
    layer_slots = placement_two[experts_two].astype(jnp.int32)
    moe_two = expert_layer(normed, layer_slots, gates_two, w_in_two, w_down_two)
    return (mixed_wide + moe_two).astype(jnp.bfloat16)
```

```python
import jax
import jax.numpy as jnp
from jax import lax
from jax.sharding import PartitionSpec as P

ALL = ("ep", "dp", "tp")


def expert_weight(targets, gate_values, expert_id):
    return jnp.sum(jnp.where(targets == expert_id, gate_values, 0.0), axis=1)


def moe_dense(rows_in, targets, gate_values, w_in, w_down):
    row_width = rows_in.shape[1]
    half_width = w_down.shape[1]
    my_expert = lax.axis_index("ep") * lax.axis_size("dp") + lax.axis_index("dp")
    rows = lax.all_gather(rows_in, ALL, axis=0, tiled=True)
    targets = lax.all_gather(targets, ALL, axis=0, tiled=True)
    gate_values = lax.all_gather(gate_values, ALL, axis=0, tiled=True)
    weight = expert_weight(targets, gate_values, my_expert)
    gate_up = jnp.dot(rows, w_in.reshape(row_width, 2 * half_width), preferred_element_type=jnp.float32)
    hidden = (jax.nn.silu(gate_up[:, :half_width]) * gate_up[:, half_width:]).astype(jnp.bfloat16)
    out = jnp.dot(hidden, w_down[0], preferred_element_type=jnp.float32)
    out = (out * weight[:, None]).astype(jnp.bfloat16)
    return lax.psum_scatter(out, ALL, scatter_dimension=0, tiled=True).astype(jnp.float32)


def shards(tokens, experts_one, gates_one, w_in_one, w_down_one, norm_gain, experts_two, gates_two, placement_two, w_in_two, w_down_two):
    moe_one = moe_dense(tokens, experts_one, gates_one, w_in_one, w_down_one)
    mixed = (tokens.astype(jnp.float32) + moe_one).astype(jnp.bfloat16)
    mixed_wide = mixed.astype(jnp.float32)
    inv_rms = lax.rsqrt(jnp.mean(mixed_wide * mixed_wide, axis=1, keepdims=True) + 1e-06)
    normed = (mixed_wide * inv_rms * norm_gain[None, :]).astype(jnp.bfloat16)
    expert_range = jnp.arange(placement_two.shape[0], dtype=jnp.int32)
    matches = experts_two[:, :, None] == expert_range[None, None, :]
    layer_slots = jnp.sum(jnp.where(matches, placement_two[None, None, :], 0), axis=2)
    moe_two = moe_dense(normed, layer_slots, gates_two, w_in_two, w_down_two)
    return (mixed_wide + moe_two).astype(jnp.bfloat16)


def solution(mesh):
    rows = P(("groups", "ep", "dp", "tp"), None)
    w_in = P(("ep", "dp"), None, None, "tp")
    w_down = P(("ep", "dp"), "tp", None)
    in_specs = (rows, rows, rows, w_in, w_down, P(), rows, rows, P(), w_in, w_down)
    return jax.shard_map(shards, mesh=mesh, in_specs=in_specs, out_specs=rows, check_vma=False)
```

```python
import functools

import jax
import jax.numpy as jnp
from jax import lax
from jax.experimental import pallas as pl
from jax.experimental.pallas import tpu as pltpu
from jax.sharding import PartitionSpec as P

MESH = pl.DeviceIdType.MESH
LANES = 128


def layer_kernel(
    n, experts, width, blk, w_in_hbm, w_down_hbm, out,
    rows, part, core_in, cross, x_in, line, z_in, w_in, w_down, hidden,
    w_sem, z_send, z_recv, x_send, x_recv, c_send, c_recv, d_send, d_recv,
    rc_send, rc_recv, rx_send, rx_recv, rz_send, rz_recv,
):
    z = lax.axis_index("ep")
    d = lax.axis_index("dp")
    mine = z * lax.axis_size("dp") + d
    x_peer = {"dp": (d + 2) % 4}
    c_peer = {"dp": d + 1 - 2 * (d % 2)}
    half = w_down.shape[0]
    tok = blk.shape[0]
    order = sorted(range(n), key=lambda k: (min(k, n - k), k))

    def remote(src, dst, send, recv, to):
        return pltpu.make_async_remote_copy(
            src_ref=src, dst_ref=dst, send_sem=send, recv_sem=recv, device_id=to, device_id_type=MESH
        )

    load_in = pltpu.make_async_copy(w_in_hbm, w_in, w_sem.at[0])
    load_down = pltpu.make_async_copy(w_down_hbm, w_down, w_sem.at[1])
    load_in.start()
    load_down.start()

    barrier = pltpu.get_barrier_semaphore()
    for k in range(1, n):
        pl.semaphore_signal(barrier, inc=1, device_id={"ep": (z + k) % n}, device_id_type=MESH)
    pl.semaphore_signal(barrier, inc=1, device_id=x_peer, device_id_type=MESH)
    pl.semaphore_signal(barrier, inc=1, device_id=c_peer, device_id_type=MESH)
    pl.semaphore_wait(barrier, n + 1)

    sends = []

    def go(copy):
        copy.start()
        sends.append(copy)
        return copy

    z_copy = {}
    for k in order[1:]:
        z_copy[k] = go(remote(blk, rows.at[k, 0], z_send.at[k], z_recv.at[k], {"ep": (z + n - k) % n}))
    x_copy, c_copy, d_copy = {}, {}, {}

    def spread(k):
        src = blk if k == 0 else rows.at[k, 0]
        x_copy[k] = go(remote(src, rows.at[k, 1], x_send.at[k], x_recv.at[k], x_peer))
        c_copy[k] = go(remote(src, rows.at[k, 2], c_send.at[k], c_recv.at[k], c_peer))

    spread(0)
    rows[0, 0] = blk[...]
    rc_copy, rx_copy, rz_copy = {}, {}, {}

    def finish(k):
        rx_copy[k].wait_recv()
        total = (
            part[k, 0].astype(jnp.float32) + core_in[k, 0].astype(jnp.float32) + x_in[k].astype(jnp.float32)
        )
        if k == 0:
            out[...] = total
        else:
            line[k] = total.astype(line.dtype)
            rz_copy[n - k] = go(
                remote(line.at[k], z_in.at[n - k], rz_send.at[k], rz_recv.at[n - k], {"ep": (z + k) % n})
            )

    for i, k in enumerate(order):
        x_copy[k].wait_recv()
        d_copy[k] = go(remote(rows.at[k, 1], rows.at[k, 3], d_send.at[k], d_recv.at[k], c_peer))
        if i + 1 < n:
            later = order[i + 1]
            z_copy[later].wait_recv()
            spread(later)
        c_copy[k].wait_recv()
        d_copy[k].wait_recv()
        if i == 0:
            load_in.wait()
            load_down.wait()
        gates = rows[k, :, :, width:].reshape(4 * tok, LANES).astype(jnp.float32)
        lane = lax.broadcasted_iota(jnp.int32, (4 * tok, LANES), 1)
        weight = jnp.sum(jnp.where((lane == mine) | (lane == mine + experts), gates, 0.0), axis=1, keepdims=True)
        step = 256 if half % 256 == 0 else LANES

        @pl.loop(0, half // step)
        def _(j):
            x = rows[k, :, :, :width].reshape(4 * tok, width)
            at = pl.multiple_of(j * step, step)
            gate = jnp.dot(x, w_in[:, pl.ds(at, step)], preferred_element_type=jnp.float32)
            up = jnp.dot(x, w_in[:, pl.ds(half + at, step)], preferred_element_type=jnp.float32)
            hidden[:, pl.ds(at, step)] = (gate / (1.0 + jnp.exp(-gate)) * up).astype(hidden.dtype)

        wide = 256 if width % 256 == 0 else LANES

        @pl.loop(0, width // wide)
        def _(j):
            at = pl.multiple_of(j * wide, wide)
            y = jnp.dot(hidden[...], w_down[:, pl.ds(at, wide)], preferred_element_type=jnp.float32)
            y = jnp.where(weight == 0.0, 0.0, y * weight)
            part[k, :, :, pl.ds(at, wide)] = y.astype(part.dtype).reshape(4, tok, wide)

        rc_copy[k] = go(remote(part.at[k, pl.ds(2, 2)], core_in.at[k], rc_send.at[k], rc_recv.at[k], c_peer))
        if i > 0:
            finish(order[i - 1])
        rc_copy[k].wait_recv()
        cross[k] = (part[k, 1].astype(jnp.float32) + core_in[k, 1].astype(jnp.float32)).astype(cross.dtype)
        rx_copy[k] = go(remote(cross.at[k], x_in.at[k], rx_send.at[k], rx_recv.at[k], x_peer))
    finish(order[-1])
    for k in order[1:]:
        rz_copy[k].wait_recv()
        out[...] += z_in[k].astype(jnp.float32)
    for copy in sends:
        copy.wait_send()


def expert_layer(block, w_in, w_down, experts, number):
    tok, wide = block.shape
    half, width = w_down.shape[1:]
    n = lax.axis_size("ep")
    bf16 = jnp.bfloat16
    dma = pltpu.SemaphoreType.DMA
    return pl.pallas_call(
        functools.partial(layer_kernel, n, experts, width),
        out_shape=jax.ShapeDtypeStruct((tok, width), jnp.float32),
        in_specs=[
            pl.BlockSpec(memory_space=pltpu.VMEM),
            pl.BlockSpec(memory_space=pl.ANY),
            pl.BlockSpec(memory_space=pl.ANY),
        ],
        out_specs=pl.BlockSpec(memory_space=pltpu.VMEM),
        scratch_shapes=[
            pltpu.VMEM((n, 4, tok, wide), bf16),
            pltpu.VMEM((n, 4, tok, width), bf16),
            pltpu.VMEM((n, 2, tok, width), bf16),
            pltpu.VMEM((n, tok, width), bf16),
            pltpu.VMEM((n, tok, width), bf16),
            pltpu.VMEM((n, tok, width), bf16),
            pltpu.VMEM((n, tok, width), bf16),
            pltpu.VMEM((width, 2 * half), bf16),
            pltpu.VMEM((half, width), bf16),
            pltpu.VMEM((4 * tok, half), bf16),
            dma((2,)),
        ]
        + [dma((n,))] * 14,
        compiler_params=pltpu.CompilerParams(
            collective_id=number, has_side_effects=True, vmem_limit_bytes=56 * 1024 * 1024
        ),
        name=f"layer_{number}",
    )(block, w_in.reshape(width, 2 * half), w_down.reshape(half, width))


def with_gates(rows_in, targets, gate_values, experts):
    matches = targets[:, :, None] == jnp.arange(experts, dtype=jnp.int32)[None, None, :]
    table = jnp.sum(jnp.where(matches, gate_values[:, :, None], 0.0), axis=1)
    high = table.astype(jnp.bfloat16)
    low = (table - high.astype(jnp.float32)).astype(jnp.bfloat16)
    rest = jnp.zeros((rows_in.shape[0], LANES - 2 * experts), jnp.bfloat16)
    return jnp.concatenate([rows_in, high, low, rest], axis=1)


def fused_shards(
    tokens, experts_one, gates_one, w_in_one, w_down_one, norm_gain,
    experts_two, gates_two, placement_two, w_in_two, w_down_two,
):
    experts = placement_two.shape[0]
    expert_range = jnp.arange(experts, dtype=jnp.int32)
    matches = experts_two[:, :, None] == expert_range[None, None, :]
    layer_slots = jnp.sum(jnp.where(matches, placement_two[None, None, :], 0), axis=2)
    moe_one = expert_layer(with_gates(tokens, experts_one, gates_one, experts), w_in_one, w_down_one, experts, 0)
    mixed = (tokens.astype(jnp.float32) + moe_one).astype(jnp.bfloat16)
    mixed_wide = mixed.astype(jnp.float32)
    inv_rms = lax.rsqrt(jnp.mean(mixed_wide * mixed_wide, axis=1, keepdims=True) + 1e-06)
    normed = (mixed_wide * inv_rms * norm_gain[None, :]).astype(jnp.bfloat16)
    moe_two = expert_layer(with_gates(normed, layer_slots, gates_two, experts), w_in_two, w_down_two, experts, 1)
    return (mixed_wide + moe_two).astype(jnp.bfloat16)


def capacity(tok_rows, top_count, expert_count):
    return max(2, min(tok_rows, 5 * tok_rows * top_count // (4 * expert_count)))


def pack_rows(rows_in, targets, expert_count, per_slot):
    tok_rows, top_count = targets.shape
    flat_ids = targets.reshape(-1)
    hit_table = (flat_ids[:, None] == jnp.arange(expert_count, dtype=jnp.int32)[None, :]).astype(
        jnp.int32
    )
    before = jnp.cumsum(hit_table, axis=0) - hit_table
    slot_rank = jnp.sum(before * hit_table, axis=1)
    slot_index = flat_ids * per_slot + slot_rank
    source = jnp.arange(tok_rows * top_count, dtype=jnp.int32) // top_count
    owner_row = jnp.zeros((expert_count * per_slot,), jnp.int32).at[slot_index].set(source)
    filled = jnp.zeros((expert_count * per_slot,), jnp.int32).at[slot_index].set(1)
    buffer = jnp.where(filled[:, None] > 0, rows_in[owner_row], jnp.zeros((), rows_in.dtype))
    return (buffer, slot_index)


def to_experts(buffer, expert_count, per_slot):
    row_width = buffer.shape[1]
    arrived = lax.all_to_all(
        buffer.reshape(expert_count, per_slot, row_width),
        ("ep", "dp"),
        split_axis=0,
        concat_axis=0,
        tiled=True,
    )
    return arrived.reshape(expert_count * per_slot, row_width)


def to_owners(produced, expert_count, per_slot):
    row_width = produced.shape[1]
    returned = lax.all_to_all(
        produced.reshape(expert_count, per_slot, row_width),
        ("ep", "dp"),
        split_axis=0,
        concat_axis=0,
        tiled=True,
    )
    return returned.reshape(expert_count * per_slot, row_width)


def run_expert(received, w_in, w_down):
    row_width = received.shape[1]
    down_local = w_down[0]
    half_width = down_local.shape[0]
    w_local = w_in.reshape(row_width, 2 * half_width)
    gate_up = jnp.dot(
        lax.all_gather(received, "tp", axis=0, tiled=True),
        w_local,
        preferred_element_type=jnp.float32,
    )
    hidden = (jax.nn.silu(gate_up[:, :half_width]) * gate_up[:, half_width:]).astype(jnp.bfloat16)
    return lax.psum_scatter(
        jnp.dot(hidden, down_local, preferred_element_type=jnp.float32).astype(jnp.bfloat16),
        "tp",
        scatter_dimension=0,
        tiled=True,
    )


def moe_block(rows_in, targets, gate_values, w_in, w_down, expert_count, per_slot):
    tok_rows, top_count = targets.shape
    row_width = rows_in.shape[1]
    buffer, slot_index = pack_rows(rows_in, targets, expert_count, per_slot)
    arrived = to_experts(buffer, expert_count, per_slot)
    produced = run_expert(arrived, w_in, w_down)
    returned = to_owners(produced, expert_count, per_slot)
    picked = returned[slot_index].reshape(tok_rows, top_count, row_width)
    return jnp.sum(gate_values[:, :, None] * picked.astype(jnp.float32), axis=1)


def shards(
    tokens,
    experts_one,
    gates_one,
    w_in_one,
    w_down_one,
    norm_gain,
    experts_two,
    gates_two,
    placement_two,
    w_in_two,
    w_down_two,
):
    tok_rows, top_count = experts_one.shape
    expert_count = placement_two.shape[0]
    per_slot = capacity(tok_rows, top_count, expert_count)
    moe_one = moe_block(
        tokens, experts_one, gates_one, w_in_one, w_down_one, expert_count, per_slot
    )
    mixed = (tokens.astype(jnp.float32) + moe_one).astype(jnp.bfloat16)
    mixed = lax.optimization_barrier(mixed)
    mixed_wide = mixed.astype(jnp.float32)
    inv_rms = lax.rsqrt(jnp.mean(mixed_wide * mixed_wide, axis=1, keepdims=True) + 1e-06)
    normed = (mixed_wide * inv_rms * norm_gain[None, :]).astype(jnp.bfloat16)
    expert_range = jnp.arange(expert_count, dtype=jnp.int32)
    matches = experts_two[:, :, None] == expert_range[None, None, :]
    layer_slots = jnp.sum(jnp.where(matches, placement_two[None, None, :], 0), axis=2)
    moe_two = moe_block(
        normed, layer_slots, gates_two, w_in_two, w_down_two, expert_count, per_slot
    )
    return (mixed_wide + moe_two).astype(jnp.bfloat16)


def solution(mesh):
    in_specs = (
        P(("groups", "ep", "dp", "tp"), None),
        P(("groups", "ep", "dp", "tp"), None),
        P(("groups", "ep", "dp", "tp"), None),
        P(("ep", "dp"), None, None, "tp"),
        P(("ep", "dp"), "tp", None),
        P(),
        P(("groups", "ep", "dp", "tp"), None),
        P(("groups", "ep", "dp", "tp"), None),
        P(),
        P(("ep", "dp"), None, None, "tp"),
        P(("ep", "dp"), "tp", None),
    )
    out_specs = P(("groups", "ep", "dp", "tp"), None)
    fused = mesh.shape["tp"] == 1 and mesh.shape["dp"] == 4 and mesh.shape["ep"] <= 4
    return jax.shard_map(fused_shards if fused else shards, mesh=mesh, in_specs=in_specs, out_specs=out_specs, check_vma=False)
```

```python
import functools

import jax
import jax.numpy as jnp
from jax import lax
from jax.experimental import pallas as pl
from jax.experimental.pallas import tpu as pltpu
from jax.sharding import PartitionSpec as P

MESH = pl.DeviceIdType.MESH
LANES = 128


def layer_kernel(
    n, experts, width, blk, w_in_hbm, w_down_hbm, out,
    rows, part, core_in, cross, x_in, line, z_in, w_in, w_down, hidden,
    w_sem, z_send, z_recv, x_send, x_recv, c_send, c_recv, d_send, d_recv,
    rc_send, rc_recv, rx_send, rx_recv, rz_send, rz_recv,
):
    z = lax.axis_index("ep")
    d = lax.axis_index("dp")
    mine = z * lax.axis_size("dp") + d
    x_peer = {"dp": (d + 2) % 4}
    c_peer = {"dp": d + 1 - 2 * (d % 2)}
    half = w_down.shape[0]
    tok = blk.shape[0]
    pair = z + 1 - 2 * (z % 2)
    order = [z, pair, 2 - z // 2, 3 - 3 * (z // 2)]
    inner = z % 3 != 0

    def remote(src, dst, send, recv, to):
        return pltpu.make_async_remote_copy(
            src_ref=src, dst_ref=dst, send_sem=send, recv_sem=recv, device_id=to, device_id_type=MESH
        )

    load_in = pltpu.make_async_copy(w_in_hbm, w_in, w_sem.at[0])
    load_down = pltpu.make_async_copy(w_down_hbm, w_down, w_sem.at[1])
    load_in.start()
    load_down.start()

    barrier = pltpu.get_barrier_semaphore()
    for k in range(1, n):
        pl.semaphore_signal(barrier, inc=1, device_id={"ep": (z + k) % n}, device_id_type=MESH)
    pl.semaphore_signal(barrier, inc=1, device_id=x_peer, device_id_type=MESH)
    pl.semaphore_signal(barrier, inc=1, device_id=c_peer, device_id_type=MESH)
    pl.semaphore_wait(barrier, n + 1)

    sends = []

    def go(copy):
        copy.start()
        sends.append(copy)
        return copy

    up = remote(blk, rows.at[z, 0], z_send.at[0], z_recv.at[z], {"ep": (z + 1) % n})
    down = remote(blk, rows.at[z, 0], z_send.at[n], z_recv.at[z], {"ep": (z + n - 1) % n})
    has_up, has_down = z < n - 1, z > 0
    pl.when(has_up)(up.start)
    pl.when(has_down)(down.start)
    x_copy, c_copy, d_copy, passed = {}, {}, {}, {}

    def spread(i):
        b = order[i]
        src = blk if i == 0 else rows.at[b, 0]
        x_copy[i] = go(remote(src, rows.at[b, 1], x_send.at[i], x_recv.at[i], x_peer))
        if i > 0:
            to = {"ep": 3 - z if i == 1 else pair}
            passed[i] = remote(src, rows.at[b, 0], z_send.at[i], z_recv.at[b], to)
            pl.when(inner)(passed[i].start)
        c_copy[i] = go(remote(src, rows.at[b, 2], c_send.at[i], c_recv.at[i], c_peer))

    spread(0)
    rows[z, 0] = blk[...]
    rc_copy, rx_copy, rz_copy = {}, {}, {}

    def to_cross(i):
        rc_copy[i].wait_recv()
        cross[i] = (part[i, 1].astype(jnp.float32) + core_in[i, 1].astype(jnp.float32)).astype(cross.dtype)
        rx_copy[i] = go(remote(cross.at[i], x_in.at[i], rx_send.at[i], rx_recv.at[i], x_peer))

    def finish(i):
        rx_copy[i].wait_recv()
        total = (
            part[i, 0].astype(jnp.float32) + core_in[i, 0].astype(jnp.float32) + x_in[i].astype(jnp.float32)
        )
        if i == 0:
            out[...] = total
        else:
            line[i] = total.astype(line.dtype)
            go(remote(line.at[i], z_in.at[z], rz_send.at[i], rz_recv.at[z], {"ep": order[i]}))

    for i, b in enumerate(order):
        x_copy[i].wait_recv()
        d_copy[i] = go(remote(rows.at[b, 1], rows.at[b, 3], d_send.at[i], d_recv.at[i], c_peer))
        if i + 1 < n:
            later = order[i + 1]
            remote(blk, rows.at[later, 0], z_send.at[0], z_recv.at[later], {"ep": pair}).wait_recv()
            spread(i + 1)
        c_copy[i].wait_recv()
        d_copy[i].wait_recv()
        if i == 0:
            load_in.wait()
            load_down.wait()
        gates = rows[b, :, :, width:].reshape(4 * tok, LANES).astype(jnp.float32)
        lane = lax.broadcasted_iota(jnp.int32, (4 * tok, LANES), 1)
        weight = jnp.sum(jnp.where((lane == mine) | (lane == mine + experts), gates, 0.0), axis=1, keepdims=True)
        step = 256 if half % 256 == 0 else LANES

        @pl.loop(0, half // step)
        def _(j):
            x = rows[b, :, :, :width].reshape(4 * tok, width)
            at = pl.multiple_of(j * step, step)
            gate = jnp.dot(x, w_in[:, pl.ds(at, step)], preferred_element_type=jnp.float32)
            up_part = jnp.dot(x, w_in[:, pl.ds(half + at, step)], preferred_element_type=jnp.float32)
            hidden[:, pl.ds(at, step)] = (gate / (1.0 + jnp.exp(-gate)) * up_part).astype(hidden.dtype)

        wide = 256 if width % 256 == 0 else LANES

        @pl.loop(0, width // wide)
        def _(j):
            at = pl.multiple_of(j * wide, wide)
            y = jnp.dot(hidden[...], w_down[:, pl.ds(at, wide)], preferred_element_type=jnp.float32)
            y = jnp.where(weight == 0.0, 0.0, y * weight)
            part[i, :, :, pl.ds(at, wide)] = y.astype(part.dtype).reshape(4, tok, wide)

        rc_copy[i] = go(remote(part.at[i, pl.ds(2, 2)], core_in.at[i], rc_send.at[i], rc_recv.at[i], c_peer))
        if i > 0:
            to_cross(i)
        if i > 1:
            finish(i - 1)
    to_cross(0)
    finish(n - 1)
    finish(0)
    for i in range(1, n):
        b = order[i]
        remote(line.at[i], z_in.at[b], rz_send.at[0], rz_recv.at[b], {"ep": b}).wait_recv()
        out[...] += z_in[b].astype(jnp.float32)
    pl.when(has_up)(up.wait_send)
    pl.when(has_down)(down.wait_send)
    for copy in passed.values():
        pl.when(inner)(copy.wait_send)
    for copy in sends:
        copy.wait_send()


def expert_layer(block, w_in, w_down, experts, number):
    tok, wide = block.shape
    half, width = w_down.shape[1:]
    n = lax.axis_size("ep")
    bf16 = jnp.bfloat16
    dma = pltpu.SemaphoreType.DMA
    return pl.pallas_call(
        functools.partial(layer_kernel, n, experts, width),
        out_shape=jax.ShapeDtypeStruct((tok, width), jnp.float32),
        in_specs=[
            pl.BlockSpec(memory_space=pltpu.VMEM),
            pl.BlockSpec(memory_space=pl.ANY),
            pl.BlockSpec(memory_space=pl.ANY),
        ],
        out_specs=pl.BlockSpec(memory_space=pltpu.VMEM),
        scratch_shapes=[
            pltpu.VMEM((n, 4, tok, wide), bf16),
            pltpu.VMEM((n, 4, tok, width), bf16),
            pltpu.VMEM((n, 2, tok, width), bf16),
            pltpu.VMEM((n, tok, width), bf16),
            pltpu.VMEM((n, tok, width), bf16),
            pltpu.VMEM((n, tok, width), bf16),
            pltpu.VMEM((n, tok, width), bf16),
            pltpu.VMEM((width, 2 * half), bf16),
            pltpu.VMEM((half, width), bf16),
            pltpu.VMEM((4 * tok, half), bf16),
            dma((2,)),
            dma((n + 1,)),
        ]
        + [dma((n,))] * 13,
        compiler_params=pltpu.CompilerParams(
            collective_id=number, has_side_effects=True, vmem_limit_bytes=56 * 1024 * 1024
        ),
        name=f"layer_{number}",
    )(block, w_in.reshape(width, 2 * half), w_down.reshape(half, width))


def with_gates(rows_in, targets, gate_values, experts):
    matches = targets[:, :, None] == jnp.arange(experts, dtype=jnp.int32)[None, None, :]
    table = jnp.sum(jnp.where(matches, gate_values[:, :, None], 0.0), axis=1)
    high = table.astype(jnp.bfloat16)
    low = (table - high.astype(jnp.float32)).astype(jnp.bfloat16)
    rest = jnp.zeros((rows_in.shape[0], LANES - 2 * experts), jnp.bfloat16)
    return jnp.concatenate([rows_in, high, low, rest], axis=1)


def fused_shards(
    tokens, experts_one, gates_one, w_in_one, w_down_one, norm_gain,
    experts_two, gates_two, placement_two, w_in_two, w_down_two,
):
    experts = placement_two.shape[0]
    expert_range = jnp.arange(experts, dtype=jnp.int32)
    matches = experts_two[:, :, None] == expert_range[None, None, :]
    layer_slots = jnp.sum(jnp.where(matches, placement_two[None, None, :], 0), axis=2)
    moe_one = expert_layer(with_gates(tokens, experts_one, gates_one, experts), w_in_one, w_down_one, experts, 0)
    mixed = (tokens.astype(jnp.float32) + moe_one).astype(jnp.bfloat16)
    mixed_wide = mixed.astype(jnp.float32)
    inv_rms = lax.rsqrt(jnp.mean(mixed_wide * mixed_wide, axis=1, keepdims=True) + 1e-06)
    normed = (mixed_wide * inv_rms * norm_gain[None, :]).astype(jnp.bfloat16)
    moe_two = expert_layer(with_gates(normed, layer_slots, gates_two, experts), w_in_two, w_down_two, experts, 1)
    return (mixed_wide + moe_two).astype(jnp.bfloat16)


def capacity(tok_rows, top_count, expert_count):
    return max(2, min(tok_rows, 5 * tok_rows * top_count // (4 * expert_count)))


def pack_rows(rows_in, targets, expert_count, per_slot):
    tok_rows, top_count = targets.shape
    flat_ids = targets.reshape(-1)
    hit_table = (flat_ids[:, None] == jnp.arange(expert_count, dtype=jnp.int32)[None, :]).astype(
        jnp.int32
    )
    before = jnp.cumsum(hit_table, axis=0) - hit_table
    slot_rank = jnp.sum(before * hit_table, axis=1)
    slot_index = flat_ids * per_slot + slot_rank
    source = jnp.arange(tok_rows * top_count, dtype=jnp.int32) // top_count
    owner_row = jnp.zeros((expert_count * per_slot,), jnp.int32).at[slot_index].set(source)
    filled = jnp.zeros((expert_count * per_slot,), jnp.int32).at[slot_index].set(1)
    buffer = jnp.where(filled[:, None] > 0, rows_in[owner_row], jnp.zeros((), rows_in.dtype))
    return (buffer, slot_index)


def to_experts(buffer, expert_count, per_slot):
    row_width = buffer.shape[1]
    arrived = lax.all_to_all(
        buffer.reshape(expert_count, per_slot, row_width),
        ("ep", "dp"),
        split_axis=0,
        concat_axis=0,
        tiled=True,
    )
    return arrived.reshape(expert_count * per_slot, row_width)


def to_owners(produced, expert_count, per_slot):
    row_width = produced.shape[1]
    returned = lax.all_to_all(
        produced.reshape(expert_count, per_slot, row_width),
        ("ep", "dp"),
        split_axis=0,
        concat_axis=0,
        tiled=True,
    )
    return returned.reshape(expert_count * per_slot, row_width)


def run_expert(received, w_in, w_down):
    row_width = received.shape[1]
    down_local = w_down[0]
    half_width = down_local.shape[0]
    w_local = w_in.reshape(row_width, 2 * half_width)
    gate_up = jnp.dot(
        lax.all_gather(received, "tp", axis=0, tiled=True),
        w_local,
        preferred_element_type=jnp.float32,
    )
    hidden = (jax.nn.silu(gate_up[:, :half_width]) * gate_up[:, half_width:]).astype(jnp.bfloat16)
    return lax.psum_scatter(
        jnp.dot(hidden, down_local, preferred_element_type=jnp.float32).astype(jnp.bfloat16),
        "tp",
        scatter_dimension=0,
        tiled=True,
    )


def moe_block(rows_in, targets, gate_values, w_in, w_down, expert_count, per_slot):
    tok_rows, top_count = targets.shape
    row_width = rows_in.shape[1]
    buffer, slot_index = pack_rows(rows_in, targets, expert_count, per_slot)
    arrived = to_experts(buffer, expert_count, per_slot)
    produced = run_expert(arrived, w_in, w_down)
    returned = to_owners(produced, expert_count, per_slot)
    picked = returned[slot_index].reshape(tok_rows, top_count, row_width)
    return jnp.sum(gate_values[:, :, None] * picked.astype(jnp.float32), axis=1)


def shards(
    tokens,
    experts_one,
    gates_one,
    w_in_one,
    w_down_one,
    norm_gain,
    experts_two,
    gates_two,
    placement_two,
    w_in_two,
    w_down_two,
):
    tok_rows, top_count = experts_one.shape
    expert_count = placement_two.shape[0]
    per_slot = capacity(tok_rows, top_count, expert_count)
    moe_one = moe_block(
        tokens, experts_one, gates_one, w_in_one, w_down_one, expert_count, per_slot
    )
    mixed = (tokens.astype(jnp.float32) + moe_one).astype(jnp.bfloat16)
    mixed = lax.optimization_barrier(mixed)
    mixed_wide = mixed.astype(jnp.float32)
    inv_rms = lax.rsqrt(jnp.mean(mixed_wide * mixed_wide, axis=1, keepdims=True) + 1e-06)
    normed = (mixed_wide * inv_rms * norm_gain[None, :]).astype(jnp.bfloat16)
    expert_range = jnp.arange(expert_count, dtype=jnp.int32)
    matches = experts_two[:, :, None] == expert_range[None, None, :]
    layer_slots = jnp.sum(jnp.where(matches, placement_two[None, None, :], 0), axis=2)
    moe_two = moe_block(
        normed, layer_slots, gates_two, w_in_two, w_down_two, expert_count, per_slot
    )
    return (mixed_wide + moe_two).astype(jnp.bfloat16)


def solution(mesh):
    in_specs = (
        P(("groups", "ep", "dp", "tp"), None),
        P(("groups", "ep", "dp", "tp"), None),
        P(("groups", "ep", "dp", "tp"), None),
        P(("ep", "dp"), None, None, "tp"),
        P(("ep", "dp"), "tp", None),
        P(),
        P(("groups", "ep", "dp", "tp"), None),
        P(("groups", "ep", "dp", "tp"), None),
        P(),
        P(("ep", "dp"), None, None, "tp"),
        P(("ep", "dp"), "tp", None),
    )
    out_specs = P(("groups", "ep", "dp", "tp"), None)
    fused = mesh.shape["tp"] == 1 and mesh.shape["dp"] == 4 and mesh.shape["ep"] == 4
    return jax.shard_map(fused_shards if fused else shards, mesh=mesh, in_specs=in_specs, out_specs=out_specs, check_vma=False)
```

```python
import functools

import jax
import jax.numpy as jnp
from jax import lax
from jax.experimental import pallas as pl
from jax.experimental.pallas import tpu as pltpu
from jax.sharding import PartitionSpec as P

MESH = pl.DeviceIdType.MESH
LANES = 128


def layer_kernel(
    n, experts, width, blk, w_in_hbm, w_down_hbm, out,
    rows, part, core_in, cross, x_in, line, z_in, raw, w_in, w_down, hidden,
    w_sem, z_send, z_recv, x_send, x_recv, c_send, c_recv, d_send, d_recv,
    rc_send, rc_recv, rx_send, rx_recv, rz_send, rz_recv,
):
    z = lax.axis_index("ep")
    d = lax.axis_index("dp")
    mine = z * lax.axis_size("dp") + d
    x_peer = {"dp": (d + 2) % 4}
    c_peer = {"dp": d + 1 - 2 * (d % 2)}
    half = w_down.shape[0]
    tok = blk.shape[0]
    pair = z + 1 - 2 * (z % 2)
    order = [z, pair, 2 - z // 2, 3 - 3 * (z // 2)]
    inner = z % 3 != 0

    def remote(src, dst, send, recv, to):
        return pltpu.make_async_remote_copy(
            src_ref=src, dst_ref=dst, send_sem=send, recv_sem=recv, device_id=to, device_id_type=MESH
        )

    load_in = pltpu.make_async_copy(w_in_hbm, raw, w_sem.at[0])
    load_down = pltpu.make_async_copy(w_down_hbm, w_down, w_sem.at[1])
    load_in.start()
    load_down.start()

    barrier = pltpu.get_barrier_semaphore()
    for k in range(1, n):
        pl.semaphore_signal(barrier, inc=1, device_id={"ep": (z + k) % n}, device_id_type=MESH)
    pl.semaphore_signal(barrier, inc=1, device_id=x_peer, device_id_type=MESH)
    pl.semaphore_signal(barrier, inc=1, device_id=c_peer, device_id_type=MESH)
    pl.semaphore_wait(barrier, n + 1)

    sends = []

    def go(copy):
        copy.start()
        sends.append(copy)
        return copy

    size = tok // 2
    halves = [pl.ds(h * size, size) for h in range(2)]
    has_up, has_down = z < n - 1, z > 0
    outer = jnp.logical_not(inner)
    ups, downs = [], []
    for h, at in enumerate(halves):
        own = blk.at[at]
        ups.append(remote(own, rows.at[z, 0, at], z_send.at[0, h], z_recv.at[z, h], {"ep": (z + 1) % n}))
        downs.append(remote(own, rows.at[z, 0, at], z_send.at[n, h], z_recv.at[z, h], {"ep": (z + n - 1) % n}))
    x_copy, c_copy, d_copy = {}, {}, {}
    for i, b in enumerate(order):
        src = blk if i == 0 else rows.at[b, 0]
        for h, at in enumerate(halves):
            x_copy[i, h] = remote(src.at[at], rows.at[b, 1, at], x_send.at[i, h], x_recv.at[i, h], x_peer)
        c_copy[i] = remote(src, rows.at[b, 2], c_send.at[i], c_recv.at[i], c_peer)
        d_copy[i] = remote(rows.at[b, 1], rows.at[b, 3], d_send.at[i], d_recv.at[i], c_peer)
        sends += [x_copy[i, 0], x_copy[i, 1], c_copy[i], d_copy[i]]

    def arrive(i, relay):
        b = order[i]
        to = {"ep": 3 - z if i == 1 else pair}
        for h, at in enumerate(halves):
            move = remote(rows.at[b, 0, at], rows.at[b, 0, at], z_send.at[i, h], z_recv.at[b, h], to)
            move.wait_recv()
            if relay:
                pl.when(inner)(move.start)
            x_copy[i, h].start()
        c_copy[i].start()

    for h in range(2):
        pl.when(has_up)(ups[h].start)
        pl.when(has_down)(downs[h].start)
        x_copy[0, h].start()
    c_copy[0].start()
    rows[z, 0] = blk[...]
    load_in.wait()
    group = 128

    @pl.loop(0, w_in.shape[0] // group)
    def _(j):
        at = pl.ds(pl.multiple_of(j * group, group), group)
        w_in[at, :half] = raw[at, 0, :]
        w_in[at, half:] = raw[at, 1, :]

    load_down.wait()
    rc_copy, rx_copy = {}, {}

    def to_cross(i):
        rc_copy[i].wait_recv()
        for h, at in enumerate(halves):
            value = part[i, 1, at].astype(jnp.float32) + core_in[i, 1, at].astype(jnp.float32)
            cross[i, at] = value.astype(cross.dtype)
            rx_copy[i, h] = go(
                remote(cross.at[i, at], x_in.at[i, at], rx_send.at[i, h], rx_recv.at[i, h], x_peer)
            )

    def finish(i):
        for h, at in enumerate(halves):
            rx_copy[i, h].wait_recv()
            total = (
                part[i, 0, at].astype(jnp.float32)
                + core_in[i, 0, at].astype(jnp.float32)
                + x_in[i, at].astype(jnp.float32)
            )
            if i == 0:
                out[at] = total
            else:
                line[i, at] = total.astype(line.dtype)
                go(remote(line.at[i, at], z_in.at[z, at], rz_send.at[i, h], rz_recv.at[z, h], {"ep": order[i]}))

    for i, b in enumerate(order):
        if i == 0:
            arrive(1, True)
            pl.when(inner)(functools.partial(arrive, 2, True))
        elif i == 1:
            pl.when(outer)(functools.partial(arrive, 2, False))
            pl.when(inner)(functools.partial(arrive, 3, True))
        elif i == 2:
            pl.when(outer)(functools.partial(arrive, 3, False))
        for h in range(2):
            x_copy[i, h].wait_recv()
        d_copy[i].start()
        c_copy[i].wait_recv()
        d_copy[i].wait_recv()
        gates = rows[b, :, :, width:].reshape(4 * tok, LANES).astype(jnp.float32)
        lane = lax.broadcasted_iota(jnp.int32, (4 * tok, LANES), 1)
        weight = jnp.sum(jnp.where((lane == mine) | (lane == mine + experts), gates, 0.0), axis=1, keepdims=True)
        step = 256 if half % 256 == 0 else LANES

        @pl.loop(0, half // step)
        def _(j):
            x = rows[b, :, :, :width].reshape(4 * tok, width)
            at = pl.multiple_of(j * step, step)
            gate = jnp.dot(x, w_in[:, pl.ds(at, step)], preferred_element_type=jnp.float32)
            up_part = jnp.dot(x, w_in[:, pl.ds(half + at, step)], preferred_element_type=jnp.float32)
            hidden[:, pl.ds(at, step)] = (gate / (1.0 + jnp.exp(-gate)) * up_part).astype(hidden.dtype)

        wide = 256 if width % 256 == 0 else LANES

        @pl.loop(0, width // wide)
        def _(j):
            at = pl.multiple_of(j * wide, wide)
            y = jnp.dot(hidden[...], w_down[:, pl.ds(at, wide)], preferred_element_type=jnp.float32)
            y = jnp.where(weight == 0.0, 0.0, y * weight)
            part[i, :, :, pl.ds(at, wide)] = y.astype(part.dtype).reshape(4, tok, wide)

        rc_copy[i] = go(remote(part.at[i, pl.ds(2, 2)], core_in.at[i], rc_send.at[i], rc_recv.at[i], c_peer))
        if i > 0:
            to_cross(i)
        if i == n - 1:
            to_cross(0)
        if i > 1:
            finish(i - 1)
    finish(n - 1)
    finish(0)
    for i in range(1, n):
        b = order[i]
        for h, at in enumerate(halves):
            remote(line.at[i, at], z_in.at[b, at], rz_send.at[0, h], rz_recv.at[b, h], {"ep": b}).wait_recv()
            out[at] += z_in[b, at].astype(jnp.float32)
    for h in range(2):
        pl.when(has_up)(ups[h].wait_send)
        pl.when(has_down)(downs[h].wait_send)
    for i in range(1, n):
        for h, at in enumerate(halves):
            spot = rows.at[order[i], 0, at]
            pl.when(inner)(remote(spot, spot, z_send.at[i, h], z_recv.at[0, h], {"ep": pair}).wait_send)
    for copy in sends:
        copy.wait_send()


def expert_layer(block, w_in, w_down, experts, number):
    tok, wide = block.shape
    half, width = w_down.shape[1:]
    n = lax.axis_size("ep")
    bf16 = jnp.bfloat16
    dma = pltpu.SemaphoreType.DMA
    return pl.pallas_call(
        functools.partial(layer_kernel, n, experts, width),
        out_shape=jax.ShapeDtypeStruct((tok, width), jnp.float32),
        in_specs=[
            pl.BlockSpec(memory_space=pltpu.VMEM),
            pl.BlockSpec(memory_space=pl.ANY),
            pl.BlockSpec(memory_space=pl.ANY),
        ],
        out_specs=pl.BlockSpec(memory_space=pltpu.VMEM),
        scratch_shapes=[
            pltpu.VMEM((n, 4, tok, wide), bf16),
            pltpu.VMEM((n, 4, tok, width), bf16),
            pltpu.VMEM((n, 2, tok, width), bf16),
            pltpu.VMEM((n, tok, width), bf16),
            pltpu.VMEM((n, tok, width), bf16),
            pltpu.VMEM((n, tok, width), bf16),
            pltpu.VMEM((n, tok, width), bf16),
            pltpu.VMEM((width, 2, half), bf16),
            pltpu.VMEM((width, 2 * half), bf16),
            pltpu.VMEM((half, width), bf16),
            pltpu.VMEM((4 * tok, half), bf16),
            dma((2,)),
            dma((n + 1, 2)),
            dma((n, 2)),
            dma((n, 2)),
            dma((n, 2)),
        ]
        + [dma((n,))] * 6
        + [dma((n, 2))] * 4,
        compiler_params=pltpu.CompilerParams(
            collective_id=number, has_side_effects=True, vmem_limit_bytes=56 * 1024 * 1024
        ),
        name=f"layer_{number}",
    )(block, w_in.reshape(width, 2, half), w_down.reshape(half, width))


def with_gates(rows_in, targets, gate_values, experts):
    matches = targets[:, :, None] == jnp.arange(experts, dtype=jnp.int32)[None, None, :]
    table = jnp.sum(jnp.where(matches, gate_values[:, :, None], 0.0), axis=1)
    high = table.astype(jnp.bfloat16)
    low = (table - high.astype(jnp.float32)).astype(jnp.bfloat16)
    rest = jnp.zeros((rows_in.shape[0], LANES - 2 * experts), jnp.bfloat16)
    return jnp.concatenate([rows_in, high, low, rest], axis=1)


def fused_shards(
    tokens, experts_one, gates_one, w_in_one, w_down_one, norm_gain,
    experts_two, gates_two, placement_two, w_in_two, w_down_two,
):
    experts = placement_two.shape[0]
    expert_range = jnp.arange(experts, dtype=jnp.int32)
    matches = experts_two[:, :, None] == expert_range[None, None, :]
    layer_slots = jnp.sum(jnp.where(matches, placement_two[None, None, :], 0), axis=2)
    moe_one = expert_layer(with_gates(tokens, experts_one, gates_one, experts), w_in_one, w_down_one, experts, 0)
    mixed = (tokens.astype(jnp.float32) + moe_one).astype(jnp.bfloat16)
    mixed_wide = mixed.astype(jnp.float32)
    inv_rms = lax.rsqrt(jnp.mean(mixed_wide * mixed_wide, axis=1, keepdims=True) + 1e-06)
    normed = (mixed_wide * inv_rms * norm_gain[None, :]).astype(jnp.bfloat16)
    moe_two = expert_layer(with_gates(normed, layer_slots, gates_two, experts), w_in_two, w_down_two, experts, 1)
    return (mixed_wide + moe_two).astype(jnp.bfloat16)


def capacity(tok_rows, top_count, expert_count):
    return max(2, min(tok_rows, 5 * tok_rows * top_count // (4 * expert_count)))


def pack_rows(rows_in, targets, expert_count, per_slot):
    tok_rows, top_count = targets.shape
    flat_ids = targets.reshape(-1)
    hit_table = (flat_ids[:, None] == jnp.arange(expert_count, dtype=jnp.int32)[None, :]).astype(
        jnp.int32
    )
    before = jnp.cumsum(hit_table, axis=0) - hit_table
    slot_rank = jnp.sum(before * hit_table, axis=1)
    slot_index = flat_ids * per_slot + slot_rank
    source = jnp.arange(tok_rows * top_count, dtype=jnp.int32) // top_count
    owner_row = jnp.zeros((expert_count * per_slot,), jnp.int32).at[slot_index].set(source)
    filled = jnp.zeros((expert_count * per_slot,), jnp.int32).at[slot_index].set(1)
    buffer = jnp.where(filled[:, None] > 0, rows_in[owner_row], jnp.zeros((), rows_in.dtype))
    return (buffer, slot_index)


def to_experts(buffer, expert_count, per_slot):
    row_width = buffer.shape[1]
    arrived = lax.all_to_all(
        buffer.reshape(expert_count, per_slot, row_width),
        ("ep", "dp"),
        split_axis=0,
        concat_axis=0,
        tiled=True,
    )
    return arrived.reshape(expert_count * per_slot, row_width)


def to_owners(produced, expert_count, per_slot):
    row_width = produced.shape[1]
    returned = lax.all_to_all(
        produced.reshape(expert_count, per_slot, row_width),
        ("ep", "dp"),
        split_axis=0,
        concat_axis=0,
        tiled=True,
    )
    return returned.reshape(expert_count * per_slot, row_width)


def run_expert(received, w_in, w_down):
    row_width = received.shape[1]
    down_local = w_down[0]
    half_width = down_local.shape[0]
    w_local = w_in.reshape(row_width, 2 * half_width)
    gate_up = jnp.dot(
        lax.all_gather(received, "tp", axis=0, tiled=True),
        w_local,
        preferred_element_type=jnp.float32,
    )
    hidden = (jax.nn.silu(gate_up[:, :half_width]) * gate_up[:, half_width:]).astype(jnp.bfloat16)
    return lax.psum_scatter(
        jnp.dot(hidden, down_local, preferred_element_type=jnp.float32).astype(jnp.bfloat16),
        "tp",
        scatter_dimension=0,
        tiled=True,
    )


def moe_block(rows_in, targets, gate_values, w_in, w_down, expert_count, per_slot):
    tok_rows, top_count = targets.shape
    row_width = rows_in.shape[1]
    buffer, slot_index = pack_rows(rows_in, targets, expert_count, per_slot)
    arrived = to_experts(buffer, expert_count, per_slot)
    produced = run_expert(arrived, w_in, w_down)
    returned = to_owners(produced, expert_count, per_slot)
    picked = returned[slot_index].reshape(tok_rows, top_count, row_width)
    return jnp.sum(gate_values[:, :, None] * picked.astype(jnp.float32), axis=1)


def shards(
    tokens,
    experts_one,
    gates_one,
    w_in_one,
    w_down_one,
    norm_gain,
    experts_two,
    gates_two,
    placement_two,
    w_in_two,
    w_down_two,
):
    tok_rows, top_count = experts_one.shape
    expert_count = placement_two.shape[0]
    per_slot = capacity(tok_rows, top_count, expert_count)
    moe_one = moe_block(
        tokens, experts_one, gates_one, w_in_one, w_down_one, expert_count, per_slot
    )
    mixed = (tokens.astype(jnp.float32) + moe_one).astype(jnp.bfloat16)
    mixed = lax.optimization_barrier(mixed)
    mixed_wide = mixed.astype(jnp.float32)
    inv_rms = lax.rsqrt(jnp.mean(mixed_wide * mixed_wide, axis=1, keepdims=True) + 1e-06)
    normed = (mixed_wide * inv_rms * norm_gain[None, :]).astype(jnp.bfloat16)
    expert_range = jnp.arange(expert_count, dtype=jnp.int32)
    matches = experts_two[:, :, None] == expert_range[None, None, :]
    layer_slots = jnp.sum(jnp.where(matches, placement_two[None, None, :], 0), axis=2)
    moe_two = moe_block(
        normed, layer_slots, gates_two, w_in_two, w_down_two, expert_count, per_slot
    )
    return (mixed_wide + moe_two).astype(jnp.bfloat16)


def solution(mesh):
    in_specs = (
        P(("groups", "ep", "dp", "tp"), None),
        P(("groups", "ep", "dp", "tp"), None),
        P(("groups", "ep", "dp", "tp"), None),
        P(("ep", "dp"), None, None, "tp"),
        P(("ep", "dp"), "tp", None),
        P(),
        P(("groups", "ep", "dp", "tp"), None),
        P(("groups", "ep", "dp", "tp"), None),
        P(),
        P(("ep", "dp"), None, None, "tp"),
        P(("ep", "dp"), "tp", None),
    )
    out_specs = P(("groups", "ep", "dp", "tp"), None)
    ready = mesh.shape["tp"] == 1 and mesh.shape["dp"] == 4 and mesh.shape["ep"] == 4

    def body(*arrays):
        return (fused_shards if ready and arrays[0].shape[0] % 32 == 0 else shards)(*arrays)

    return jax.shard_map(body, mesh=mesh, in_specs=in_specs, out_specs=out_specs, check_vma=False)
```

```python
import functools

import jax
import jax.numpy as jnp
from jax import lax
from jax.experimental import pallas as pl
from jax.experimental.pallas import tpu as pltpu
from jax.sharding import PartitionSpec as P

MESH = pl.DeviceIdType.MESH
LANES = 128


def layer_kernel(
    n, experts, width, blk, w_in_hbm, w_down_hbm, out,
    rows, part, core_in, cross, x_in, line, z_in, raw, w_in, w_down, hidden,
    w_sem, z_send, z_recv, x_send, x_recv, c_send, c_recv, d_send, d_recv,
    rc_send, rc_recv, rx_send, rx_recv, rz_send, rz_recv,
):
    z = lax.axis_index("ep")
    d = lax.axis_index("dp")
    mine = z * lax.axis_size("dp") + d
    x_peer = {"dp": (d + 2) % 4}
    c_peer = {"dp": d + 1 - 2 * (d % 2)}
    half = w_down.shape[0]
    tok = blk.shape[0]
    pair = z + 1 - 2 * (z % 2)
    order = [z, pair, 2 - z // 2, 3 - 3 * (z // 2)]
    inner = z % 3 != 0

    def remote(src, dst, send, recv, to):
        return pltpu.make_async_remote_copy(
            src_ref=src, dst_ref=dst, send_sem=send, recv_sem=recv, device_id=to, device_id_type=MESH
        )

    load_in = pltpu.make_async_copy(w_in_hbm, raw, w_sem.at[0])
    load_down = pltpu.make_async_copy(w_down_hbm, w_down, w_sem.at[1])
    load_in.start()
    load_down.start()

    barrier = pltpu.get_barrier_semaphore()
    for k in range(1, n):
        pl.semaphore_signal(barrier, inc=1, device_id={"ep": (z + k) % n}, device_id_type=MESH)
    pl.semaphore_signal(barrier, inc=1, device_id=x_peer, device_id_type=MESH)
    pl.semaphore_signal(barrier, inc=1, device_id=c_peer, device_id_type=MESH)
    pl.semaphore_wait(barrier, n + 1)

    sends = []

    def go(copy):
        copy.start()
        sends.append(copy)
        return copy

    size = tok // 2
    halves = [pl.ds(h * size, size) for h in range(2)]
    has_up, has_down = z < n - 1, z > 0
    outer = jnp.logical_not(inner)
    ups, downs = [], []
    for h, at in enumerate(halves):
        own = blk.at[at]
        ups.append(remote(own, rows.at[z, 0, at], z_send.at[0, h], z_recv.at[z, h], {"ep": (z + 1) % n}))
        downs.append(remote(own, rows.at[z, 0, at], z_send.at[n, h], z_recv.at[z, h], {"ep": (z + n - 1) % n}))
    x_copy, c_copy, d_copy = {}, {}, {}
    for i, b in enumerate(order):
        src = blk if i == 0 else rows.at[b, 0]
        for h, at in enumerate(halves):
            x_copy[i, h] = remote(src.at[at], rows.at[b, 1, at], x_send.at[i, h], x_recv.at[i, h], x_peer)
        c_copy[i] = remote(src, rows.at[b, 2], c_send.at[i], c_recv.at[i], c_peer)
        d_copy[i] = remote(rows.at[b, 1], rows.at[b, 3], d_send.at[i], d_recv.at[i], c_peer)
        sends += [x_copy[i, 0], x_copy[i, 1], c_copy[i], d_copy[i]]

    def arrive(i, relay):
        b = order[i]
        to = {"ep": 3 - z if i == 1 else pair}
        for h, at in enumerate(halves):
            move = remote(rows.at[b, 0, at], rows.at[b, 0, at], z_send.at[i, h], z_recv.at[b, h], to)
            move.wait_recv()
            if relay:
                pl.when(inner)(move.start)
            x_copy[i, h].start()
        c_copy[i].start()

    for h in range(2):
        pl.when(has_up)(ups[h].start)
        pl.when(has_down)(downs[h].start)
        x_copy[0, h].start()
    c_copy[0].start()
    rows[z, 0] = blk[...]
    rc_copy, rx_copy = {}, {}

    def to_cross(i):
        rc_copy[i].wait_recv()
        for h, at in enumerate(halves):
            value = part[i, 1, at].astype(jnp.float32) + core_in[i, 1, at].astype(jnp.float32)
            cross[i, at] = value.astype(cross.dtype)
            rx_copy[i, h] = go(
                remote(cross.at[i, at], x_in.at[i, at], rx_send.at[i, h], rx_recv.at[i, h], x_peer)
            )

    def finish(i):
        for h, at in enumerate(halves):
            rx_copy[i, h].wait_recv()
            total = (
                part[i, 0, at].astype(jnp.float32)
                + core_in[i, 0, at].astype(jnp.float32)
                + x_in[i, at].astype(jnp.float32)
            )
            if i == 0:
                out[at] = total
            else:
                line[i, at] = total.astype(line.dtype)
                go(remote(line.at[i, at], z_in.at[z, at], rz_send.at[i, h], rz_recv.at[z, h], {"ep": order[i]}))

    for i, b in enumerate(order):
        if i == 0:
            arrive(1, True)
            pl.when(inner)(functools.partial(arrive, 2, True))
        elif i == 1:
            pl.when(outer)(functools.partial(arrive, 2, False))
            pl.when(inner)(functools.partial(arrive, 3, True))
        elif i == 2:
            pl.when(outer)(functools.partial(arrive, 3, False))
        for h in range(2):
            x_copy[i, h].wait_recv()
        d_copy[i].start()
        if i == 0:
            load_in.wait()
            group = 128

            @pl.loop(0, w_in.shape[0] // group)
            def _(j):
                at = pl.ds(pl.multiple_of(j * group, group), group)
                w_in[at] = raw[at].reshape(group, 2 * half)

            load_down.wait()
        c_copy[i].wait_recv()
        d_copy[i].wait_recv()
        gates = rows[b, :, :, width:].reshape(4 * tok, LANES).astype(jnp.float32)
        lane = lax.broadcasted_iota(jnp.int32, (4 * tok, LANES), 1)
        weight = jnp.sum(jnp.where((lane == mine) | (lane == mine + experts), gates, 0.0), axis=1, keepdims=True)
        step = 256 if half % 256 == 0 else LANES

        @pl.loop(0, half // step)
        def _(j):
            x = rows[b, :, :, :width].reshape(4 * tok, width)
            at = pl.multiple_of(j * step, step)
            gate = jnp.dot(x, w_in[:, pl.ds(at, step)], preferred_element_type=jnp.float32)
            up_part = jnp.dot(x, w_in[:, pl.ds(half + at, step)], preferred_element_type=jnp.float32)
            hidden[:, pl.ds(at, step)] = (gate / (1.0 + jnp.exp(-gate)) * up_part).astype(hidden.dtype)

        y = jnp.dot(hidden[...], w_down[...], preferred_element_type=jnp.float32)
        y = jnp.where(weight == 0.0, 0.0, y * weight)
        part[i] = y.astype(part.dtype).reshape(4, tok, width)

        rc_copy[i] = go(remote(part.at[i, pl.ds(2, 2)], core_in.at[i], rc_send.at[i], rc_recv.at[i], c_peer))
        if i > 0:
            to_cross(i)
        if i == n - 1:
            to_cross(0)
        if i > 1:
            finish(i - 1)
    finish(n - 1)
    finish(0)
    for i in range(1, n):
        b = order[i]
        for h, at in enumerate(halves):
            remote(line.at[i, at], z_in.at[b, at], rz_send.at[0, h], rz_recv.at[b, h], {"ep": b}).wait_recv()
            out[at] += z_in[b, at].astype(jnp.float32)
    for h in range(2):
        pl.when(has_up)(ups[h].wait_send)
        pl.when(has_down)(downs[h].wait_send)
    for i in range(1, n):
        for h, at in enumerate(halves):
            spot = rows.at[order[i], 0, at]
            pl.when(inner)(remote(spot, spot, z_send.at[i, h], z_recv.at[0, h], {"ep": pair}).wait_send)
    for copy in sends:
        copy.wait_send()


def expert_layer(block, w_in, w_down, experts, number):
    tok, wide = block.shape
    half, width = w_down.shape[1:]
    n = lax.axis_size("ep")
    bf16 = jnp.bfloat16
    dma = pltpu.SemaphoreType.DMA
    return pl.pallas_call(
        functools.partial(layer_kernel, n, experts, width),
        out_shape=jax.ShapeDtypeStruct((tok, width), jnp.float32),
        in_specs=[
            pl.BlockSpec(memory_space=pltpu.VMEM),
            pl.BlockSpec(memory_space=pl.ANY),
            pl.BlockSpec(memory_space=pl.ANY),
        ],
        out_specs=pl.BlockSpec(memory_space=pltpu.VMEM),
        scratch_shapes=[
            pltpu.VMEM((n, 4, tok, wide), bf16),
            pltpu.VMEM((n, 4, tok, width), bf16),
            pltpu.VMEM((n, 2, tok, width), bf16),
            pltpu.VMEM((n, tok, width), bf16),
            pltpu.VMEM((n, tok, width), bf16),
            pltpu.VMEM((n, tok, width), bf16),
            pltpu.VMEM((n, tok, width), bf16),
            pltpu.VMEM((width, 2, half), bf16),
            pltpu.VMEM((width, 2 * half), bf16),
            pltpu.VMEM((half, width), bf16),
            pltpu.VMEM((4 * tok, half), bf16),
            dma((2,)),
            dma((n + 1, 2)),
            dma((n, 2)),
            dma((n, 2)),
            dma((n, 2)),
        ]
        + [dma((n,))] * 6
        + [dma((n, 2))] * 4,
        compiler_params=pltpu.CompilerParams(
            collective_id=number, has_side_effects=True, vmem_limit_bytes=56 * 1024 * 1024
        ),
        name=f"layer_{number}",
    )(block, w_in.reshape(width, 2, half), w_down.reshape(half, width))


def with_gates(rows_in, targets, gate_values, experts):
    matches = targets[:, :, None] == jnp.arange(experts, dtype=jnp.int32)[None, None, :]
    table = jnp.sum(jnp.where(matches, gate_values[:, :, None], 0.0), axis=1)
    high = table.astype(jnp.bfloat16)
    low = (table - high.astype(jnp.float32)).astype(jnp.bfloat16)
    rest = jnp.zeros((rows_in.shape[0], LANES - 2 * experts), jnp.bfloat16)
    return jnp.concatenate([rows_in, high, low, rest], axis=1)


def fused_shards(
    tokens, experts_one, gates_one, w_in_one, w_down_one, norm_gain,
    experts_two, gates_two, placement_two, w_in_two, w_down_two,
):
    experts = placement_two.shape[0]
    expert_range = jnp.arange(experts, dtype=jnp.int32)
    matches = experts_two[:, :, None] == expert_range[None, None, :]
    layer_slots = jnp.sum(jnp.where(matches, placement_two[None, None, :], 0), axis=2)
    moe_one = expert_layer(with_gates(tokens, experts_one, gates_one, experts), w_in_one, w_down_one, experts, 0)
    mixed = (tokens.astype(jnp.float32) + moe_one).astype(jnp.bfloat16)
    mixed_wide = mixed.astype(jnp.float32)
    inv_rms = lax.rsqrt(jnp.mean(mixed_wide * mixed_wide, axis=1, keepdims=True) + 1e-06)
    normed = (mixed_wide * inv_rms * norm_gain[None, :]).astype(jnp.bfloat16)
    moe_two = expert_layer(with_gates(normed, layer_slots, gates_two, experts), w_in_two, w_down_two, experts, 1)
    return (mixed_wide + moe_two).astype(jnp.bfloat16)


def capacity(tok_rows, top_count, expert_count):
    return max(2, min(tok_rows, 5 * tok_rows * top_count // (4 * expert_count)))


def pack_rows(rows_in, targets, expert_count, per_slot):
    tok_rows, top_count = targets.shape
    flat_ids = targets.reshape(-1)
    hit_table = (flat_ids[:, None] == jnp.arange(expert_count, dtype=jnp.int32)[None, :]).astype(
        jnp.int32
    )
    before = jnp.cumsum(hit_table, axis=0) - hit_table
    slot_rank = jnp.sum(before * hit_table, axis=1)
    slot_index = flat_ids * per_slot + slot_rank
    source = jnp.arange(tok_rows * top_count, dtype=jnp.int32) // top_count
    owner_row = jnp.zeros((expert_count * per_slot,), jnp.int32).at[slot_index].set(source)
    filled = jnp.zeros((expert_count * per_slot,), jnp.int32).at[slot_index].set(1)
    buffer = jnp.where(filled[:, None] > 0, rows_in[owner_row], jnp.zeros((), rows_in.dtype))
    return (buffer, slot_index)


def to_experts(buffer, expert_count, per_slot):
    row_width = buffer.shape[1]
    arrived = lax.all_to_all(
        buffer.reshape(expert_count, per_slot, row_width),
        ("ep", "dp"),
        split_axis=0,
        concat_axis=0,
        tiled=True,
    )
    return arrived.reshape(expert_count * per_slot, row_width)


def to_owners(produced, expert_count, per_slot):
    row_width = produced.shape[1]
    returned = lax.all_to_all(
        produced.reshape(expert_count, per_slot, row_width),
        ("ep", "dp"),
        split_axis=0,
        concat_axis=0,
        tiled=True,
    )
    return returned.reshape(expert_count * per_slot, row_width)


def run_expert(received, w_in, w_down):
    row_width = received.shape[1]
    down_local = w_down[0]
    half_width = down_local.shape[0]
    w_local = w_in.reshape(row_width, 2 * half_width)
    gate_up = jnp.dot(
        lax.all_gather(received, "tp", axis=0, tiled=True),
        w_local,
        preferred_element_type=jnp.float32,
    )
    hidden = (jax.nn.silu(gate_up[:, :half_width]) * gate_up[:, half_width:]).astype(jnp.bfloat16)
    return lax.psum_scatter(
        jnp.dot(hidden, down_local, preferred_element_type=jnp.float32).astype(jnp.bfloat16),
        "tp",
        scatter_dimension=0,
        tiled=True,
    )


def moe_block(rows_in, targets, gate_values, w_in, w_down, expert_count, per_slot):
    tok_rows, top_count = targets.shape
    row_width = rows_in.shape[1]
    buffer, slot_index = pack_rows(rows_in, targets, expert_count, per_slot)
    arrived = to_experts(buffer, expert_count, per_slot)
    produced = run_expert(arrived, w_in, w_down)
    returned = to_owners(produced, expert_count, per_slot)
    picked = returned[slot_index].reshape(tok_rows, top_count, row_width)
    return jnp.sum(gate_values[:, :, None] * picked.astype(jnp.float32), axis=1)


def shards(
    tokens,
    experts_one,
    gates_one,
    w_in_one,
    w_down_one,
    norm_gain,
    experts_two,
    gates_two,
    placement_two,
    w_in_two,
    w_down_two,
):
    tok_rows, top_count = experts_one.shape
    expert_count = placement_two.shape[0]
    per_slot = capacity(tok_rows, top_count, expert_count)
    moe_one = moe_block(
        tokens, experts_one, gates_one, w_in_one, w_down_one, expert_count, per_slot
    )
    mixed = (tokens.astype(jnp.float32) + moe_one).astype(jnp.bfloat16)
    mixed = lax.optimization_barrier(mixed)
    mixed_wide = mixed.astype(jnp.float32)
    inv_rms = lax.rsqrt(jnp.mean(mixed_wide * mixed_wide, axis=1, keepdims=True) + 1e-06)
    normed = (mixed_wide * inv_rms * norm_gain[None, :]).astype(jnp.bfloat16)
    expert_range = jnp.arange(expert_count, dtype=jnp.int32)
    matches = experts_two[:, :, None] == expert_range[None, None, :]
    layer_slots = jnp.sum(jnp.where(matches, placement_two[None, None, :], 0), axis=2)
    moe_two = moe_block(
        normed, layer_slots, gates_two, w_in_two, w_down_two, expert_count, per_slot
    )
    return (mixed_wide + moe_two).astype(jnp.bfloat16)


def solution(mesh):
    in_specs = (
        P(("groups", "ep", "dp", "tp"), None),
        P(("groups", "ep", "dp", "tp"), None),
        P(("groups", "ep", "dp", "tp"), None),
        P(("ep", "dp"), None, None, "tp"),
        P(("ep", "dp"), "tp", None),
        P(),
        P(("groups", "ep", "dp", "tp"), None),
        P(("groups", "ep", "dp", "tp"), None),
        P(),
        P(("ep", "dp"), None, None, "tp"),
        P(("ep", "dp"), "tp", None),
    )
    out_specs = P(("groups", "ep", "dp", "tp"), None)
    ready = mesh.shape["tp"] == 1 and mesh.shape["dp"] == 4 and mesh.shape["ep"] == 4

    def body(*arrays):
        return (fused_shards if ready and arrays[0].shape[0] % 32 == 0 else shards)(*arrays)

    return jax.shard_map(body, mesh=mesh, in_specs=in_specs, out_specs=out_specs, check_vma=False)
```
